32 devices in a mesh: grp: 2 (over x), tile: 16 (over z, y, core).
Axes of the slice: x: 2, y: 2, z: 4, core: 2. Of those that a mesh axis runs over, the one named last changes fastest.
Arguments:
- quantized: bfloat16 [16, 96, 2048], P(None, 'grp', 'tile'), may hold values from -6 to 6
- scales: float32 [16, 16, 96], P('tile', None, 'grp'), may hold values from 0.25 to 4
Outputs:
- coefficients: bfloat16 [16, 96, 2048], P(None, 'grp', 'tile')
The draws below stay inside these ranges and needn't reach their ends.
All inputs are finite; a program needn't handle non-finite values.
Results may differ from the reference program's by a relative error of at most 0.001.
Values sent between devices are 32-bit elements; how exact they have to be, the bound alone decides.
No kernel may reach another device: no remote copies, remote signals or barrier semaphores. Data moves between devices by JAX's collectives and lax.ppermute only.
A program may use at most 64 MiB of HBM per device.

```python
import math
import jax
import jax.numpy as jnp
from jax import lax

NZ = 16
QB = 128
LEVELS = 4
NY = 96
NX = 2048


def steps_of(rng, extent, pieces, low, top_value):
    def one(dim, parts):
        steps = jax.random.uniform(jax.random.fold_in(jax.random.fold_in(rng, 6), dim), (parts,), jnp.float32, low / len(pieces), top_value / len(pieces))
        return jnp.repeat(jnp.exp(steps), extent[dim] // parts).reshape((-1,) + (1,) * (len(extent) - dim - 1))

    factor_of = one(*pieces[0])
    for cut in pieces[1:]:
        factor_of = factor_of * one(*cut)
    return factor_of


def noise(own_key, dims, scale, limit, split=(), dtype=jnp.bfloat16):
    level = steps_of(own_key, dims, split, -0.22, 0.18) if split else 1.0
    array = jax.random.normal(own_key, dims, jnp.float32) * scale * level
    return jnp.minimum(jnp.maximum(array, -limit), limit).astype(dtype)


def setup_inputs(seed: int = 0) -> dict:
    splits = jax.random.split(jax.random.key(seed), 3)
    quantized = noise(splits[0], (NZ, NY, NX), 1.0, 6.0, ((1, 2), (2, 16)))
    scales = jnp.clip(jnp.exp(math.log(4.0) - 2.7725887 * jax.random.uniform(splits[1], (NX // QB, NZ, NY), jnp.float32) ** steps_of(splits[1], (NX // QB, NZ, NY), ((0, 16), (2, 2)), -0.2, 0.2)), 0.25, 4.0)
    return dict(quantized=quantized, scales=scales)


LIFT_ALPHA = -1.586134342059924
LIFT_BETA = -0.052980118572961
LIFT_GAMMA = 0.882911075530934
LIFT_DELTA = 0.443506852043971
LIFT_KAPPA = 1.230174104914001


def forward_of(values, along):
    length = values.shape[along]
    return jnp.concatenate([lax.slice_in_dim(values, 1, length, 1, along), lax.slice_in_dim(values, length - 1, length, 1, along)], along)


def backward_of(values, along):
    length = values.shape[along]
    return jnp.concatenate([lax.slice_in_dim(values, 0, 1, 1, along), lax.slice_in_dim(values, 0, length - 1, 1, along)], along)


def lift_axis(subband, along):
    length = subband.shape[along]
    even_part = lax.slice_in_dim(subband, 0, length, 2, along)
    odd_part = lax.slice_in_dim(subband, 1, length, 2, along)
    odd_part = odd_part + LIFT_ALPHA * (even_part + forward_of(even_part, along))
    even_part = even_part + LIFT_BETA * (backward_of(odd_part, along) + odd_part)
    odd_part = odd_part + LIFT_GAMMA * (even_part + forward_of(even_part, along))
    even_part = even_part + LIFT_DELTA * (backward_of(odd_part, along) + odd_part)
    even_part = even_part / LIFT_KAPPA
    odd_part = odd_part * (LIFT_KAPPA / 2.0)
    return jnp.stack([even_part, odd_part], along + 1).reshape(subband.shape)


def decompose(subband, level_index):
    for along in (2, 1, 0):
        subband = lift_axis(subband, along)
    if level_index + 1 < LEVELS:
        coarser = decompose(subband[::2, ::2, ::2], level_index + 1)
        subband = subband.at[::2, ::2, ::2].set(coarser)
    return subband


def reference(quantized, scales):
    blocks = quantized.astype(jnp.float32).reshape(NZ, NY, NX // QB, QB)
    factor = jnp.transpose(scales, (1, 2, 0))[..., None]
    density = (blocks * factor).reshape(NZ, NY, NX)
    return decompose(density, 0).astype(jnp.bfloat16)
```

```python
import numpy as np
import jax
import jax.numpy as jnp
from jax import lax
from jax.experimental import pallas as pl
from jax.experimental.pallas import tpu as pltpu
from jax.sharding import PartitionSpec as P

LEVELS = 4
LANES = 128

LIFT_ALPHA = -1.586134342059924
LIFT_BETA = -0.052980118572961
LIFT_GAMMA = 0.882911075530934
LIFT_DELTA = 0.443506852043971
LIFT_KAPPA = 1.230174104914001


def lift_matrix(m):
    e, o = m[0::2], m[1::2]
    after = lambda v: np.concatenate([v[1:], v[-1:]])
    before = lambda v: np.concatenate([v[:1], v[:-1]])
    o = o + LIFT_ALPHA * (e + after(e))
    e = e + LIFT_BETA * (before(o) + o)
    o = o + LIFT_GAMMA * (e + after(e))
    e = e + LIFT_DELTA * (before(o) + o)
    return np.stack([e / LIFT_KAPPA, o * (LIFT_KAPPA / 2.0)], 1).reshape(m.shape)


def operators(length):
    low, ops = np.eye(length), []
    for _ in range(LEVELS):
        full = lift_matrix(low)
        ops.append(full)
        low = full[0::2]
    return ops


def factor(block):
    rest, us, vs = block.copy(), [], []
    top = np.abs(block).max()
    while top > 0 and np.abs(rest).max() > 1e-12 * top:
        i, j = np.unravel_index(np.argmax(np.abs(rest)), rest.shape)
        u, v = rest[:, j] / rest[i, j], rest[i].copy()
        rest = rest - u[:, None] * v[None]
        us.append(u)
        vs.append(v)
    rows, cols = block.shape
    return (
        np.stack(us, 1) if us else np.zeros((rows, 0)),
        np.stack(vs, 0) if vs else np.zeros((0, cols)),
    )


class Plan:
    def __init__(self, count, block):
        assert count == 1 or count % 2 == 0
        long = block >= 2 * sum(4 << l for l in range(LEVELS))
        kinds = min(count, 4) if long else count
        self.count, self.block, self.kinds = count, block, kinds
        ops = operators(kinds * block)
        size = [block >> l for l in range(LEVELS)]
        cut = lambda l, q, p: ops[l][q * size[l] : (q + 1) * size[l], p * block : (p + 1) * block]
        self.own = [[cut(l, p, p) for l in range(LEVELS)] for p in range(kinds)]
        moves = [lambda p: p ^ 1, lambda p: ((p + 1) ^ 1) - 1]
        for hop in range(2, kinds):
            moves += [lambda p, hop=hop: p + hop, lambda p, hop=hop: p - hop]
        self.perms, self.rank, self.u, self.v = [], [], [], []
        for move in moves:
            pairs = [(p, move(p)) for p in range(kinds) if 0 <= move(p) < kinds]
            parts = {pq: [factor(cut(l, pq[1], pq[0])) for l in range(LEVELS)] for pq in pairs}
            rank = [max([f[l][0].shape[1] for f in parts.values()] + [0]) for l in range(LEVELS)]
            if not sum(rank):
                continue
            assert max(rank) <= 8
            u = [[np.zeros((size[l], rank[l])) for l in range(LEVELS)] for _ in range(kinds)]
            v = [[np.zeros((rank[l], block)) for l in range(LEVELS)] for _ in range(kinds)]
            for (p, q), fs in parts.items():
                for l, (fu, fv) in enumerate(fs):
                    u[q][l][:, : fu.shape[1]] = fu
                    v[p][l][: fv.shape[0]] = fv
            self.perms.append([(p, move(p)) for p in range(count) if 0 <= move(p) < count])
            self.rank.append(rank)
            self.u.append(u)
            self.v.append(v)

    def kind(self, axis):
        p = lax.axis_index(axis)
        if self.kinds == self.count:
            return p
        return jnp.where(p == 0, 0, jnp.where(p == self.count - 1, 3, 2 - lax.rem(p, 2)))


def up(n, m):
    return -(-n // m) * m


def split_np(m):
    hi = m.astype(jnp.bfloat16)
    return hi, (m - hi.astype(np.float64)).astype(jnp.bfloat16)


def split(x):
    hi = x.astype(jnp.bfloat16)
    return hi, (x - hi.astype(jnp.float32)).astype(jnp.bfloat16)


def lift_planes(planes):
    e, o = planes[0::2], planes[1::2]
    n = len(e)
    after = lambda v, i: v[min(i + 1, n - 1)]
    before = lambda v, i: v[max(i - 1, 0)]
    o = [o[i] + LIFT_ALPHA * (e[i] + after(e, i)) for i in range(n)]
    e = [e[i] + LIFT_BETA * (before(o, i) + o[i]) for i in range(n)]
    o = [o[i] + LIFT_GAMMA * (e[i] + after(e, i)) for i in range(n)]
    e = [e[i] + LIFT_DELTA * (before(o, i) + o[i]) for i in range(n)]
    out = []
    for i in range(n):
        out += [e[i] * (1.0 / LIFT_KAPPA), o[i] * (LIFT_KAPPA / 2.0)]
    return out


def mm(a, b, dims):
    return lax.dot_general(a, b, (dims, ((), ())), preferred_element_type=jnp.float32)


NN, NT, TN = ((1,), (0,)), ((1,), (1,)), ((0,), (0,))
VMEM = pl.BlockSpec(memory_space=pltpu.VMEM)


def call(kernel, outs, args, scratch=(), flops=0, specs=None):
    moved = sum(int(np.prod(a.shape)) * a.dtype.itemsize for a in list(args) + list(outs))
    many = len(outs) > 1
    return pl.pallas_call(
        kernel,
        out_shape=tuple(outs) if many else outs[0],
        in_specs=specs or [VMEM] * len(args),
        out_specs=(VMEM,) * len(outs) if many else VMEM,
        scratch_shapes=list(scratch),
        cost_estimate=pl.CostEstimate(flops=flops, bytes_accessed=moved, transcendentals=0),
    )(*args)


def body_of(ny, nx):
    def body(quantized, scales):
        nz, rows, cols = quantized.shape
        assert scales.shape == (1, nz, rows) and cols == LANES
        assert nz % (1 << LEVELS) == 0 and rows % 8 == 0 and (nz * rows) % LANES == 0
        f32, bf16 = jnp.float32, jnp.bfloat16
        yplan, xplan = Plan(ny, rows), Plan(nx, cols)
        ey, ex = range(len(yplan.perms)), range(len(xplan.perms))
        lv = range(LEVELS)
        planes = [nz >> l for l in lv]
        height = [rows >> l for l in lv]
        base = [sum(planes[i] * height[i] for i in range(l)) for l in range(LEVELS + 1)]
        total = up(base[-1], LANES)
        chunks, chunks0 = total // LANES, base[1] // LANES

        yoff = [sum(up(height[i], 8) for i in range(l)) for l in range(LEVELS + 1)]
        yown = np.zeros((yplan.kinds, yoff[-1], rows), np.float32)
        ucoef = np.zeros((yplan.kinds, yoff[-1], LANES), np.float32)
        voff, at = {}, 0
        for l in lv:
            for e in ey:
                voff[e, l] = at
                at += yplan.rank[e][l]
        vmat = np.zeros((yplan.kinds, up(at, 8), rows), np.float32)
        for p in range(yplan.kinds):
            for l in lv:
                yown[p, yoff[l] : yoff[l] + height[l]] = yplan.own[p][l]
                for e in ey:
                    r = yplan.rank[e][l]
                    vmat[p, voff[e, l] : voff[e, l] + r] = yplan.v[e][p][l]
                    ucoef[p, yoff[l] : yoff[l] + height[l], 8 * e : 8 * e + r] = yplan.u[e][p][l]
        mbase = [[sum(planes[i] * yplan.rank[e][i] for i in range(l)) for l in range(LEVELS + 1)] for e in ey]
        mrows = [up(mbase[e][-1], 8) for e in ey]

        ne = len(xplan.perms)
        r0 = max([xplan.rank[e][0] for e in ex] + [1])
        xrows0 = up(r0 * chunks0, 8)
        xmsg = xrows0 + 8 * (chunks - chunks0)
        k0 = up(ne * r0, 8)
        s0 = np.zeros((xplan.kinds, 2 * k0, LANES), np.float32)
        s1 = np.zeros((xplan.kinds, 2 * ne * (LEVELS - 1) * 8, LANES), np.float32)
        half1 = ne * (LEVELS - 1) * 8
        kr = up(3 * k0, 16)
        ur0 = np.zeros((xplan.kinds, kr, LANES), np.float32)
        k1 = up(ne * 8, 16)
        ur1 = np.zeros((xplan.kinds, LEVELS - 1, 3 * k1, LANES), np.float32)
        xown = np.zeros((xplan.kinds, LEVELS, 3, LANES, LANES), np.float32)
        f = lambda m: np.asarray(m, np.float32)
        for p in range(xplan.kinds):
            for l in lv:
                step = 1 << l
                placed = np.zeros((LANES, LANES))
                placed[:, ::step] = xplan.own[p][l].T
                hi, lo = split_np(placed)
                xown[p, l] = np.stack([f(hi), f(hi), f(lo)])
                for e in ex:
                    r = xplan.rank[e][l]
                    vh, vl = split_np(xplan.v[e][p][l])
                    um = np.zeros((r, LANES))
                    um[:, ::step] = xplan.u[e][p][l].T
                    uh, ul = split_np(um)
                    if l == 0:
                        s0[p, e * r0 : e * r0 + r] = f(vh)
                        s0[p, k0 + e * r0 : k0 + e * r0 + r] = f(vl)
                        for j, w in enumerate((uh, uh, ul)):
                            ur0[p, j * k0 + e * r0 : j * k0 + e * r0 + r] = f(w)
                    else:
                        o = (e * (LEVELS - 1) + l - 1) * 8
                        s1[p, o : o + r] = f(vh)
                        s1[p, half1 + o : half1 + o + r] = f(vl)
                        for j, w in enumerate((uh, uh, ul)):
                            ur1[p, l - 1, j * k1 + e * 8 : j * k1 + e * 8 + r] = f(w)
        tab = lambda m, t: jnp.asarray(m.astype(t))

        def scaled(mat, s, q):
            hi, lo = split(mat * s)
            out = mm(jnp.concatenate([hi, lo], 0), q, NN)
            return out[: mat.shape[0]] + out[mat.shape[0] :]

        def k_send_y(q_ref, s_ref, v_ref, *outs):
            v = v_ref[yplan.kind("grp")]
            part = [scaled(v, s_ref[0, z : z + 1, :], q_ref[z]) for z in range(nz)]
            for l in lv:
                part = lift_planes(part)
                for e in ey:
                    r, o = yplan.rank[e][l], voff[e, l]
                    for k in range(planes[l]):
                        if r:
                            outs[e][mbase[e][l] + k * r : mbase[e][l] + (k + 1) * r, :] = part[k][o : o + r]
                part = part[0::2]
            for e in ey:
                if mrows[e] > mbase[e][-1]:
                    outs[e][mbase[e][-1] :, :] = jnp.zeros((mrows[e] - mbase[e][-1], LANES), f32)

        def k_own_yz(q_ref, s_ref, y_ref, d_ref, t_ref):
            y = y_ref[yplan.kind("grp")]
            for z in range(nz):
                t_ref[z] = scaled(y, s_ref[0, z : z + 1, :], q_ref[z])
            for l in lv:
                for t in range(yoff[l], yoff[l + 1], 8):
                    part = [t_ref[z, t : t + 8, :] for z in range(nz)]
                    for _ in range(l):
                        part = lift_planes(part)[0::2]
                    part = lift_planes(part)
                    n = min(8, yoff[l] + height[l] - t)
                    for k in range(planes[l]):
                        o = base[l] + k * height[l] + t - yoff[l]
                        d_ref[o : o + n, :] = part[k][:n]
            if total > base[-1]:
                d_ref[base[-1] :, :] = jnp.zeros((total - base[-1], LANES), f32)

        def k_send_x(d_ref, *refs):
            ms, (u_ref, s0_ref, s1_ref) = refs[: len(ey)], refs[len(ey) : len(ey) + 3]
            o_ref, outs = refs[len(ey) + 3], refs[len(ey) + 4 :]
            p = yplan.kind("grp")
            for l in lv:
                for t in range(0, height[l], 8):
                    n = min(8, height[l] - t)
                    u = u_ref[p, yoff[l] + t : yoff[l] + t + n, :]
                    cs = {(e, i): u[:, 8 * e + i : 8 * e + i + 1] for e in ey for i in range(yplan.rank[e][l])}
                    cs = {key: jnp.broadcast_to(c, (n, LANES)) for key, c in cs.items()}
                    for k in range(planes[l]):
                        o = base[l] + k * height[l] + t
                        acc = d_ref[o : o + n, :]
                        for (e, i), c in cs.items():
                            row = mbase[e][l] + k * yplan.rank[e][l] + i
                            acc = acc + c * ms[e][row : row + 1, :]
                        o_ref[o : o + n, :] = acc
            if total > base[-1]:
                o_ref[base[-1] :, :] = jnp.zeros((total - base[-1], LANES), f32)
            px = xplan.kind("tile")
            a0, a1 = s0_ref[px], s1_ref[px]
            a0, a1 = jnp.concatenate([a0, a0], 1), jnp.concatenate([a1, a1], 1)
            lane = lax.broadcasted_iota(jnp.int32, (8, LANES), 1)
            for c in range(chunks):
                d = jnp.concatenate(split(o_ref[c * LANES : (c + 1) * LANES, :]), 1)
                if c < chunks0:
                    m = mm(a0, d, NT)
                    m = m[:k0] + m[k0:]
                    for e in ex:
                        outs[e][r0 * c : r0 * (c + 1), :] = m[e * r0 : (e + 1) * r0]
                else:
                    m = mm(a1, d, NT)
                    m = m[:half1] + m[half1:]
                    for e in ex:
                        o = e * (LEVELS - 1) * 8
                        val = m[o : o + 8]
                        for l in range(2, LEVELS):
                            val = jnp.where(lane + c * LANES >= base[l], m[o + (l - 1) * 8 : o + l * 8], val)
                        w = xrows0 + 8 * (c - chunks0)
                        outs[e][w : w + 8, :] = val
            for e in ex:
                if xrows0 > r0 * chunks0:
                    outs[e][r0 * chunks0 : xrows0, :] = jnp.zeros((xrows0 - r0 * chunks0, LANES), f32)

        def k_own_x(d_ref, x_ref, o_ref, x_vmem, sem):
            copy = pltpu.make_async_copy(x_ref.at[xplan.kind("tile")], x_vmem, sem)
            copy.start()
            copy.wait()
            for l in lv:
                end = base[l + 1] if l + 1 < LEVELS else total
                hi, lo = split(d_ref[base[l] : end, :])
                o_ref[base[l] : end, :] = mm(jnp.concatenate([hi, lo, hi], 1), x_vmem[l], NN)

        def k_join(f_ref, *refs):
            ms, (u0_ref, u1_ref, out_ref, acc, low) = refs[: len(ex)], refs[len(ex) :]
            px = xplan.kind("tile")
            u0 = u0_ref[px]
            for c in range(chunks0):
                rows_in = [ms[e][r0 * c : r0 * (c + 1), :] for e in ex]
                if k0 > ne * r0:
                    rows_in.append(jnp.zeros((k0 - ne * r0, LANES), f32))
                m = jnp.concatenate(rows_in, 0)
                hi, lo = split(m)
                parts = [hi.astype(f32), lo.astype(f32), hi.astype(f32)]
                if kr > 3 * k0:
                    parts.append(jnp.zeros((kr - 3 * k0, LANES), f32))
                lhs = jnp.concatenate(parts, 0).astype(bf16)
                acc[c * LANES : (c + 1) * LANES, :] = f_ref[c * LANES : (c + 1) * LANES, :] + mm(lhs, u0, TN)
            for c in range(chunks0, chunks):
                w = xrows0 + 8 * (c - chunks0)
                rows_in = [ms[e][w : w + 8, :] for e in ex]
                if k1 > 8 * ne:
                    rows_in.append(jnp.zeros((k1 - 8 * ne, LANES), f32))
                hi, lo = split(jnp.concatenate(rows_in, 0))
                lhs = jnp.concatenate([hi, lo, hi], 0)
                for l in range(1, LEVELS):
                    a = max(base[l], c * LANES)
                    end = base[l + 1] if l + 1 < LEVELS else total
                    b = min(end, (c + 1) * LANES)
                    if a < b:
                        m = mm(lhs, u1_ref[px, l - 1], TN)
                        low[a - base[1] : b - base[1], :] = f_ref[a:b, :] + m[a - c * LANES : b - c * LANES]
            for l in range(1, LEVELS):
                step, h = 1 << l, height[l]
                lane = lax.broadcasted_iota(jnp.int32, (h, LANES), 1)
                for k in range(planes[l]):
                    o = base[l] - base[1] + k * h
                    at = pl.ds(k * step * rows, h, stride=step)
                    acc[at, :] = jnp.where(lane % step == 0, low[o : o + h, :], acc[at, :])
            for z in range(nz):
                out_ref[z] = acc[z * rows : (z + 1) * rows, :].astype(bf16)

        shape = jax.ShapeDtypeStruct
        sent = call(
            k_send_y,
            [shape((mrows[e], LANES), f32) for e in ey],
            [quantized, scales, tab(vmat, f32)],
            flops=1000000,
        )
        sent = sent if isinstance(sent, (tuple, list)) else [sent]
        got = [lax.ppermute(sent[e], "grp", yplan.perms[e]) for e in ey]
        d = call(
            k_own_yz,
            [shape((total, LANES), f32)],
            [quantized, scales, tab(yown, f32)],
            [pltpu.VMEM((nz, yoff[-1], LANES), f32)],
            flops=100000000,
        )
        d, *sent = call(
            k_send_x,
            [shape((total, LANES), f32)] + [shape((xmsg, LANES), f32) for e in ex],
            [d, *got, tab(ucoef, f32), tab(s0, bf16), tab(s1, bf16)],
            flops=10000000,
        )
        got = [lax.ppermute(sent[e], "tile", xplan.perms[e]) for e in ex]
        xtab = tab(xown.reshape(xplan.kinds, LEVELS, 3 * LANES, LANES), bf16)
        full = call(
            k_own_x,
            [shape((total, LANES), f32)],
            [d, xtab],
            [pltpu.VMEM((LEVELS, 3 * LANES, LANES), bf16), pltpu.SemaphoreType.DMA],
            flops=100000000,
            specs=[VMEM, pl.BlockSpec(memory_space=pl.ANY)],
        )
        return call(
            k_join,
            [shape(quantized.shape, bf16)],
            [full, *got, tab(ur0, bf16), tab(ur1, bf16)],
            [pltpu.VMEM((base[1], LANES), f32), pltpu.VMEM((total - base[1], LANES), f32)],
            flops=10000000,
        )

    return body


def solution(mesh):
    return jax.shard_map(
        body_of(mesh.shape["grp"], mesh.shape["tile"]),
        mesh=mesh,
        in_specs=(P(None, "grp", "tile"), P("tile", None, "grp")),
        out_specs=P(None, "grp", "tile"),
        check_vma=False,
    )
```

```python
import numpy as np
import jax
import jax.numpy as jnp
from jax import lax
from jax.experimental import pallas as pl
from jax.experimental.pallas import tpu as pltpu
from jax.sharding import PartitionSpec as P

LEVELS = 4
LANES = 128

LIFT_ALPHA = -1.586134342059924
LIFT_BETA = -0.052980118572961
LIFT_GAMMA = 0.882911075530934
LIFT_DELTA = 0.443506852043971
LIFT_KAPPA = 1.230174104914001


def lift_matrix(m):
    e, o = m[0::2], m[1::2]
    after = lambda v: np.concatenate([v[1:], v[-1:]])
    before = lambda v: np.concatenate([v[:1], v[:-1]])
    o = o + LIFT_ALPHA * (e + after(e))
    e = e + LIFT_BETA * (before(o) + o)
    o = o + LIFT_GAMMA * (e + after(e))
    e = e + LIFT_DELTA * (before(o) + o)
    return np.stack([e / LIFT_KAPPA, o * (LIFT_KAPPA / 2.0)], 1).reshape(m.shape)


def operators(length):
    low, ops = np.eye(length), []
    for _ in range(LEVELS):
        full = lift_matrix(low)
        ops.append(full)
        low = full[0::2]
    return ops


def factor(block):
    rest, us, vs = block.copy(), [], []
    top = np.abs(block).max()
    while top > 0 and np.abs(rest).max() > 1e-12 * top:
        i, j = np.unravel_index(np.argmax(np.abs(rest)), rest.shape)
        u, v = rest[:, j] / rest[i, j], rest[i].copy()
        rest = rest - u[:, None] * v[None]
        us.append(u)
        vs.append(v)
    rows, cols = block.shape
    return (
        np.stack(us, 1) if us else np.zeros((rows, 0)),
        np.stack(vs, 0) if vs else np.zeros((0, cols)),
    )


class Plan:
    def __init__(self, count, block):
        assert count == 1 or count % 2 == 0
        long = block >= 2 * sum(4 << l for l in range(LEVELS))
        kinds = min(count, 4) if long else count
        self.count, self.block, self.kinds = count, block, kinds
        ops = operators(kinds * block)
        size = [block >> l for l in range(LEVELS)]
        cut = lambda l, q, p: ops[l][q * size[l] : (q + 1) * size[l], p * block : (p + 1) * block]
        self.own = [[cut(l, p, p) for l in range(LEVELS)] for p in range(kinds)]
        moves = [lambda p: p ^ 1, lambda p: ((p + 1) ^ 1) - 1]
        for hop in range(2, kinds):
            moves += [lambda p, hop=hop: p + hop, lambda p, hop=hop: p - hop]
        self.perms, self.rank, self.u, self.v = [], [], [], []
        for move in moves:
            pairs = [(p, move(p)) for p in range(kinds) if 0 <= move(p) < kinds]
            parts = {pq: [factor(cut(l, pq[1], pq[0])) for l in range(LEVELS)] for pq in pairs}
            rank = [max([f[l][0].shape[1] for f in parts.values()] + [0]) for l in range(LEVELS)]
            if not sum(rank):
                continue
            assert max(rank) <= 8
            u = [[np.zeros((size[l], rank[l])) for l in range(LEVELS)] for _ in range(kinds)]
            v = [[np.zeros((rank[l], block)) for l in range(LEVELS)] for _ in range(kinds)]
            for (p, q), fs in parts.items():
                for l, (fu, fv) in enumerate(fs):
                    u[q][l][:, : fu.shape[1]] = fu
                    v[p][l][: fv.shape[0]] = fv
            self.perms.append([(p, move(p)) for p in range(count) if 0 <= move(p) < count])
            self.rank.append(rank)
            self.u.append(u)
            self.v.append(v)

    def kind(self, axis):
        p = lax.axis_index(axis)
        if self.kinds == self.count:
            return p
        return jnp.where(p == 0, 0, jnp.where(p == self.count - 1, 3, 2 - lax.rem(p, 2)))


def up(n, m):
    return -(-n // m) * m


def split_np(m):
    hi = m.astype(jnp.bfloat16)
    return hi, (m - hi.astype(np.float64)).astype(jnp.bfloat16)


def split(x):
    hi = x.astype(jnp.bfloat16)
    return hi, (x - hi.astype(jnp.float32)).astype(jnp.bfloat16)


def lift_planes(planes):
    e, o = planes[0::2], planes[1::2]
    n = len(e)
    after = lambda v, i: v[min(i + 1, n - 1)]
    before = lambda v, i: v[max(i - 1, 0)]
    o = [o[i] + LIFT_ALPHA * (e[i] + after(e, i)) for i in range(n)]
    e = [e[i] + LIFT_BETA * (before(o, i) + o[i]) for i in range(n)]
    o = [o[i] + LIFT_GAMMA * (e[i] + after(e, i)) for i in range(n)]
    e = [e[i] + LIFT_DELTA * (before(o, i) + o[i]) for i in range(n)]
    out = []
    for i in range(n):
        out += [e[i] * (1.0 / LIFT_KAPPA), o[i] * (LIFT_KAPPA / 2.0)]
    return out


def mm(a, b, dims):
    return lax.dot_general(a, b, (dims, ((), ())), preferred_element_type=jnp.float32)


NN, NT, TN = ((1,), (0,)), ((1,), (1,)), ((0,), (0,))
VMEM = pl.BlockSpec(memory_space=pltpu.VMEM)
HBM = pl.BlockSpec(memory_space=pltpu.HBM)


def call(kernel, outs, args, scratch=(), flops=0, hbm=0):
    moved = sum(int(np.prod(a.shape)) * a.dtype.itemsize for a in list(args) + list(outs))
    many = len(outs) > 1
    stay = len(args) - hbm
    args = list(args[:stay]) + [pltpu.with_memory_space_constraint(a, pltpu.HBM) for a in args[stay:]]
    return pl.pallas_call(
        kernel,
        out_shape=tuple(outs) if many else outs[0],
        in_specs=[VMEM] * stay + [HBM] * hbm,
        out_specs=(VMEM,) * len(outs) if many else VMEM,
        scratch_shapes=list(scratch),
        cost_estimate=pl.CostEstimate(flops=flops, bytes_accessed=moved, transcendentals=0),
        compiler_params=pltpu.CompilerParams(vmem_limit_bytes=8 << 20),
    )(*args)


def fetch(sem, *pairs):
    copies = [pltpu.make_async_copy(a, b, sem.at[i]) for i, (a, b) in enumerate(pairs)]
    for c in copies:
        c.start()
    return copies


def body_of(ny, nx):
    def body(quantized, scales):
        nz, rows, cols = quantized.shape
        assert scales.shape == (1, nz, rows) and cols == LANES
        assert nz % (1 << LEVELS) == 0 and rows % 8 == 0 and (nz * rows) % LANES == 0
        f32, bf16 = jnp.float32, jnp.bfloat16
        yplan, xplan = Plan(ny, rows), Plan(nx, cols)
        ey, ex = range(len(yplan.perms)), range(len(xplan.perms))
        lv = range(LEVELS)
        planes = [nz >> l for l in lv]
        height = [rows >> l for l in lv]
        base = [sum(planes[i] * height[i] for i in range(l)) for l in range(LEVELS + 1)]
        total = up(base[-1], LANES)
        chunks, chunks0 = total // LANES, base[1] // LANES

        yoff = [sum(up(height[i], 8) for i in range(l)) for l in range(LEVELS + 1)]
        yown = np.zeros((yplan.kinds, yoff[-1], rows), np.float32)
        ucoef = np.zeros((yplan.kinds, yoff[-1], LANES), np.float32)
        voff, at = {}, 0
        for l in lv:
            for e in ey:
                voff[e, l] = at
                at += yplan.rank[e][l]
        vmat = np.zeros((yplan.kinds, up(at, 8), rows), np.float32)
        for p in range(yplan.kinds):
            for l in lv:
                yown[p, yoff[l] : yoff[l] + height[l]] = yplan.own[p][l]
                for e in ey:
                    r = yplan.rank[e][l]
                    vmat[p, voff[e, l] : voff[e, l] + r] = yplan.v[e][p][l]
                    ucoef[p, yoff[l] : yoff[l] + height[l], 8 * e : 8 * e + r] = yplan.u[e][p][l]
        mbase = [[sum(planes[i] * yplan.rank[e][i] for i in range(l)) for l in range(LEVELS + 1)] for e in ey]
        mrows = [up(mbase[e][-1], 8) for e in ey]

        ne = len(xplan.perms)
        r0 = max([xplan.rank[e][0] for e in ex] + [1])
        xrows0 = up(r0 * chunks0, 8)
        xmsg = xrows0 + 8 * (chunks - chunks0)
        k0 = up(ne * r0, 8)
        s0 = np.zeros((xplan.kinds, 2 * k0, LANES), np.float32)
        s1 = np.zeros((xplan.kinds, 2 * ne * (LEVELS - 1) * 8, LANES), np.float32)
        half1 = ne * (LEVELS - 1) * 8
        kr = up(3 * k0, 16)
        ur0 = np.zeros((xplan.kinds, kr, LANES), np.float32)
        k1 = up(ne * 8, 16)
        ur1 = np.zeros((xplan.kinds, LEVELS - 1, 3 * k1, LANES), np.float32)
        xown = np.zeros((xplan.kinds, LEVELS, 3, LANES, LANES), np.float32)
        f = lambda m: np.asarray(m, np.float32)
        for p in range(xplan.kinds):
            for l in lv:
                step = 1 << l
                placed = np.zeros((LANES, LANES))
                placed[:, ::step] = xplan.own[p][l].T
                hi, lo = split_np(placed)
                xown[p, l] = np.stack([f(hi), f(hi), f(lo)])
                for e in ex:
                    r = xplan.rank[e][l]
                    vh, vl = split_np(xplan.v[e][p][l])
                    um = np.zeros((r, LANES))
                    um[:, ::step] = xplan.u[e][p][l].T
                    uh, ul = split_np(um)
                    if l == 0:
                        s0[p, e * r0 : e * r0 + r] = f(vh)
                        s0[p, k0 + e * r0 : k0 + e * r0 + r] = f(vl)
                        for j, w in enumerate((uh, uh, ul)):
                            ur0[p, j * k0 + e * r0 : j * k0 + e * r0 + r] = f(w)
                    else:
                        o = (e * (LEVELS - 1) + l - 1) * 8
                        s1[p, o : o + r] = f(vh)
                        s1[p, half1 + o : half1 + o + r] = f(vl)
                        for j, w in enumerate((uh, uh, ul)):
                            ur1[p, l - 1, j * k1 + e * 8 : j * k1 + e * 8 + r] = f(w)
        tab = lambda m, t: jnp.asarray(m.astype(t))

        def scaled(mat, s, q):
            hi, lo = split(mat * s)
            out = mm(jnp.concatenate([hi, lo], 0), q, NN)
            return out[: mat.shape[0]] + out[mat.shape[0] :]

        def k_send_y(q_hbm, s_hbm, v_hbm, y_hbm, *refs):
            outs, (q_ref, s_ref, y_ref, v_ref, sem) = refs[: len(ey)], refs[len(ey) :]
            p = yplan.kind("grp")
            copies = fetch(sem, (q_hbm, q_ref), (s_hbm, s_ref), (v_hbm.at[p], v_ref), (y_hbm.at[p], y_ref))
            for c in copies[:3]:
                c.wait()
            v = v_ref[...]
            part = [scaled(v, s_ref[0, z : z + 1, :], q_ref[z]) for z in range(nz)]
            for l in lv:
                part = lift_planes(part)
                for e in ey:
                    r, o = yplan.rank[e][l], voff[e, l]
                    for k in range(planes[l]):
                        if r:
                            outs[e][mbase[e][l] + k * r : mbase[e][l] + (k + 1) * r, :] = part[k][o : o + r]
                part = part[0::2]
            for e in ey:
                if mrows[e] > mbase[e][-1]:
                    outs[e][mbase[e][-1] :, :] = jnp.zeros((mrows[e] - mbase[e][-1], LANES), f32)
            copies[3].wait()

        def k_own_yz(q_ref, s_ref, y_ref, *refs):
            tables, (d_ref, *kept), (t_ref, sem) = refs[:ntab], refs[ntab : 2 * ntab + 1], refs[2 * ntab + 1 :]
            p, px = yplan.kind("grp"), xplan.kind("tile")
            kinds = [p] + [px] * (ntab - 1)
            copies = fetch(sem, *[(t.at[i], k) for t, i, k in zip(tables, kinds, kept)])
            y = y_ref[...]
            for z in range(nz):
                t_ref[z] = scaled(y, s_ref[0, z : z + 1, :], q_ref[z])
            for l in lv:
                for t in range(yoff[l], yoff[l + 1], 8):
                    part = [t_ref[z, t : t + 8, :] for z in range(nz)]
                    for _ in range(l):
                        part = lift_planes(part)[0::2]
                    part = lift_planes(part)
                    n = min(8, yoff[l] + height[l] - t)
                    for k in range(planes[l]):
                        o = base[l] + k * height[l] + t - yoff[l]
                        d_ref[o : o + n, :] = part[k][:n]
            if total > base[-1]:
                d_ref[base[-1] :, :] = jnp.zeros((total - base[-1], LANES), f32)
            for c in copies:
                c.wait()

        def k_send_x(d_ref, *refs):
            ms, (u_ref, s0_ref, s1_ref) = refs[: len(ey)], refs[len(ey) : len(ey) + 3]
            o_ref, outs = refs[len(ey) + 3], refs[len(ey) + 4 :]
            for l in lv:
                for t in range(0, height[l], 8):
                    n = min(8, height[l] - t)
                    u = u_ref[yoff[l] + t : yoff[l] + t + n, :]
                    cs = {(e, i): u[:, 8 * e + i : 8 * e + i + 1] for e in ey for i in range(yplan.rank[e][l])}
                    cs = {key: jnp.broadcast_to(c, (n, LANES)) for key, c in cs.items()}
                    for k in range(planes[l]):
                        o = base[l] + k * height[l] + t
                        acc = d_ref[o : o + n, :]
                        for (e, i), c in cs.items():
                            row = mbase[e][l] + k * yplan.rank[e][l] + i
                            acc = acc + c * ms[e][row : row + 1, :]
                        o_ref[o : o + n, :] = acc
            if total > base[-1]:
                o_ref[base[-1] :, :] = jnp.zeros((total - base[-1], LANES), f32)
            a0, a1 = s0_ref[...], s1_ref[...]
            a0, a1 = jnp.concatenate([a0, a0], 1), jnp.concatenate([a1, a1], 1)
            lane = lax.broadcasted_iota(jnp.int32, (8, LANES), 1)
            for c in range(chunks):
                d = jnp.concatenate(split(o_ref[c * LANES : (c + 1) * LANES, :]), 1)
                if c < chunks0:
                    m = mm(a0, d, NT)
                    m = m[:k0] + m[k0:]
                    for e in ex:
                        outs[e][r0 * c : r0 * (c + 1), :] = m[e * r0 : (e + 1) * r0]
                else:
                    m = mm(a1, d, NT)
                    m = m[:half1] + m[half1:]
                    for e in ex:
                        o = e * (LEVELS - 1) * 8
                        val = m[o : o + 8]
                        for l in range(2, LEVELS):
                            val = jnp.where(lane + c * LANES >= base[l], m[o + (l - 1) * 8 : o + l * 8], val)
                        w = xrows0 + 8 * (c - chunks0)
                        outs[e][w : w + 8, :] = val
            for e in ex:
                if xrows0 > r0 * chunks0:
                    outs[e][r0 * chunks0 : xrows0, :] = jnp.zeros((xrows0 - r0 * chunks0, LANES), f32)

        def k_own_x(d_ref, x_ref, o_ref):
            for l in lv:
                end = base[l + 1] if l + 1 < LEVELS else total
                hi, lo = split(d_ref[base[l] : end, :])
                o_ref[base[l] : end, :] = mm(jnp.concatenate([hi, lo, hi], 1), x_ref[l], NN)

        def k_join(f_ref, *refs):
            ms, (u0_ref, u1_ref, out_ref, acc, low) = refs[: len(ex)], refs[len(ex) :]
            u0 = u0_ref[...]
            for c in range(chunks0):
                rows_in = [ms[e][r0 * c : r0 * (c + 1), :] for e in ex]
                if k0 > ne * r0:
                    rows_in.append(jnp.zeros((k0 - ne * r0, LANES), f32))
                m = jnp.concatenate(rows_in, 0)
                hi, lo = split(m)
                parts = [hi.astype(f32), lo.astype(f32), hi.astype(f32)]
                if kr > 3 * k0:
                    parts.append(jnp.zeros((kr - 3 * k0, LANES), f32))
                lhs = jnp.concatenate(parts, 0).astype(bf16)
                acc[c * LANES : (c + 1) * LANES, :] = f_ref[c * LANES : (c + 1) * LANES, :] + mm(lhs, u0, TN)
            for c in range(chunks0, chunks):
                w = xrows0 + 8 * (c - chunks0)
                rows_in = [ms[e][w : w + 8, :] for e in ex]
                if k1 > 8 * ne:
                    rows_in.append(jnp.zeros((k1 - 8 * ne, LANES), f32))
                hi, lo = split(jnp.concatenate(rows_in, 0))
                lhs = jnp.concatenate([hi, lo, hi], 0)
                for l in range(1, LEVELS):
                    a = max(base[l], c * LANES)
                    end = base[l + 1] if l + 1 < LEVELS else total
                    b = min(end, (c + 1) * LANES)
                    if a < b:
                        m = mm(lhs, u1_ref[l - 1], TN)
                        low[a - base[1] : b - base[1], :] = f_ref[a:b, :] + m[a - c * LANES : b - c * LANES]
            for l in range(1, LEVELS):
                step, h = 1 << l, height[l]
                lane = lax.broadcasted_iota(jnp.int32, (h, LANES), 1)
                for k in range(planes[l]):
                    o = base[l] - base[1] + k * h
                    at = pl.ds(k * step * rows, h, stride=step)
                    acc[at, :] = jnp.where(lane % step == 0, low[o : o + h, :], acc[at, :])
            for z in range(nz):
                out_ref[z] = acc[z * rows : (z + 1) * rows, :].astype(bf16)

        shape = jax.ShapeDtypeStruct
        like = lambda a: shape(a.shape, a.dtype)
        one = lambda a: shape(a.shape[1:], a.dtype)
        xtab = tab(xown.reshape(xplan.kinds, LEVELS, 3 * LANES, LANES), bf16)
        tables = [tab(ucoef, f32), tab(s0, bf16), tab(s1, bf16), xtab, tab(ur0, bf16), tab(ur1, bf16)]
        ntab = len(tables)
        vtab, ytab = tab(vmat, f32), tab(yown, f32)
        *sent, q, s, y = call(
            k_send_y,
            [shape((mrows[e], LANES), f32) for e in ey] + [like(quantized), like(scales), one(ytab)],
            [quantized, scales, vtab, ytab],
            [pltpu.VMEM(vtab.shape[1:], f32), pltpu.SemaphoreType.DMA((4,))],
            flops=1000000,
            hbm=4,
        )
        got = [lax.ppermute(sent[e], "grp", yplan.perms[e]) for e in ey]
        d, u, a0, a1, xt, u0, u1 = call(
            k_own_yz,
            [shape((total, LANES), f32)] + [one(t) for t in tables],
            [q, s, y, *tables],
            [pltpu.VMEM((nz, yoff[-1], LANES), f32), pltpu.SemaphoreType.DMA((ntab,))],
            flops=100000000,
            hbm=ntab,
        )
        d, *sent = call(
            k_send_x,
            [shape((total, LANES), f32)] + [shape((xmsg, LANES), f32) for e in ex],
            [d, *got, u, a0, a1],
            flops=10000000,
        )
        got = [lax.ppermute(sent[e], "tile", xplan.perms[e]) for e in reversed(ex)][::-1]
        full = call(k_own_x, [shape((total, LANES), f32)], [d, xt], flops=100000000)
        return call(
            k_join,
            [shape(quantized.shape, bf16)],
            [full, *got, u0, u1],
            [pltpu.VMEM((base[1], LANES), f32), pltpu.VMEM((total - base[1], LANES), f32)],
            flops=10000000,
        )

    return body


def solution(mesh):
    return jax.shard_map(
        body_of(mesh.shape["grp"], mesh.shape["tile"]),
        mesh=mesh,
        in_specs=(P(None, "grp", "tile"), P("tile", None, "grp")),
        out_specs=P(None, "grp", "tile"),
        check_vma=False,
    )
```
